32 devices in a mesh: graph: 2 (over x), col: 4 (over z), row: 4 (over y, core).
Axes of the slice: x: 2, y: 2, z: 4, core: 2. Of those that a mesh axis runs over, the one named last changes fastest.
Arguments:
- a_rows: int32 [8, 4, 65536], P(('graph', 'row'), 'col'), parts along dimension 0
- a_cols: int32 [8, 4, 65536], P(('graph', 'row'), 'col'), parts along dimension 0
- a_vals: float32 [8, 4, 65536], P(('graph', 'row'), 'col'), parts along dimension 0
- a_count: int32 [8, 4], P(('graph', 'row'), 'col'), parts along dimension 0
- h_feat: bfloat16 [32768, 200], P(('graph', 'row'), 'col'), parts along dimension 0
- w_mat: bfloat16 [200, 512], P('col')
- dz_out: float32 [32768, 512], P(('graph', 'row'), 'col'), parts along dimension 0
Outputs:
- output 1: float32 [32768, 512], P(('graph', 'row'), 'col'), parts along dimension 0
- output 2: float32 [400, 512], P(('graph', 'col')), parts along dimension 0
- output 3: float32 [32768, 200], P(('graph', 'row'), 'col'), parts along dimension 0
There are 2 independent parts. The reference program is written for one: setup_inputs(seed, part) draws one part's arguments, and reference() takes and returns one part's arrays. A program takes and returns all parts, laid end to end along the dimension named above; an argument that names none is the same for every part.
All inputs are finite; a program needn't handle non-finite values.
Results may differ from the reference program's by a relative error of at most 0.00342.
Values are sent between devices in bfloat16 or wider.
A program may use at most 1 GiB of HBM per device.

```python
import jax
import jax.numpy as jnp
from jax import lax

GRID_SIDE = 4
BLOCK_ROWS = 4096
NNZ_CAP = 65536
FEAT_IN = 200
FEAT_OUT = 512
NODES = GRID_SIDE * BLOCK_ROWS


def draw_structure(struct_key):
    key_list = jax.random.split(struct_key, 10)
    grid_shape = (GRID_SIDE, GRID_SIDE)
    entry_shape = (GRID_SIDE, GRID_SIDE, NNZ_CAP)
    levels = jax.random.randint(key_list[0], grid_shape, 0, 7, dtype=jnp.int32)
    level_cap = jnp.right_shift(jnp.full(grid_shape, NNZ_CAP, jnp.int32), levels)
    jitter = jax.random.randint(key_list[1], grid_shape, 0, level_cap // 8 + 1, dtype=jnp.int32)
    peak_block = jax.random.randint(key_list[2], (), 0, GRID_SIDE * GRID_SIDE, dtype=jnp.int32)
    block_ids = jnp.arange(GRID_SIDE * GRID_SIDE, dtype=jnp.int32).reshape(grid_shape)
    counts = jnp.where(block_ids == peak_block, jnp.int32(NNZ_CAP), level_cap - jitter).astype(jnp.int32)
    row_first = jax.random.randint(key_list[3], entry_shape, 0, BLOCK_ROWS, dtype=jnp.int32)
    row_second = jax.random.randint(key_list[4], entry_shape, 0, BLOCK_ROWS, dtype=jnp.int32)
    row_shift = jax.random.randint(key_list[5], (GRID_SIDE, 1, 1), 0, BLOCK_ROWS, dtype=jnp.int32)
    col_first = jax.random.randint(key_list[6], entry_shape, 0, BLOCK_ROWS, dtype=jnp.int32)
    col_second = jax.random.randint(key_list[7], entry_shape, 0, BLOCK_ROWS, dtype=jnp.int32)
    col_shift = jax.random.randint(key_list[8], (1, GRID_SIDE, 1), 0, BLOCK_ROWS, dtype=jnp.int32)
    local_rows = ((row_first * row_second) // BLOCK_ROWS + row_shift) % BLOCK_ROWS
    local_cols = ((col_first * col_second) // BLOCK_ROWS + col_shift) % BLOCK_ROWS
    return local_rows.astype(jnp.int32), local_cols.astype(jnp.int32), counts


def setup_inputs(seed: int = 0, part: int = 0) -> dict:
    base_key = jax.random.key(seed)
    shared_key, graph_key = jax.random.split(base_key)
    part_key = jax.random.fold_in(graph_key, part)
    struct_key, value_key = jax.random.split(part_key)
    local_rows, local_cols, counts = draw_structure(struct_key)
    key_list = jax.random.split(value_key, 4)
    val_scale = BLOCK_ROWS / (GRID_SIDE * counts.astype(jnp.float32))
    a_vals = jax.random.uniform(key_list[0], (GRID_SIDE, GRID_SIDE, NNZ_CAP), jnp.float32, 0.5, 1.5) * val_scale[:, :, None]
    block_mean = jax.random.normal(key_list[1], (GRID_SIDE, 1, FEAT_IN), jnp.float32)
    node_noise = jax.random.normal(key_list[2], (GRID_SIDE, BLOCK_ROWS, FEAT_IN), jnp.float32)
    h_feat = (node_noise + block_mean).reshape(NODES, FEAT_IN).astype(jnp.bfloat16)
    w_mat = (jax.random.normal(shared_key, (FEAT_IN, FEAT_OUT), jnp.float32) * FEAT_IN ** -0.5).astype(jnp.bfloat16)
    dz_out = jax.random.normal(key_list[3], (NODES, FEAT_OUT), jnp.float32)
    return {'a_rows': local_rows, 'a_cols': local_cols, 'a_vals': a_vals, 'a_count': counts, 'h_feat': h_feat, 'w_mat': w_mat, 'dz_out': dz_out}


def block_sum(dense_blocks, out_lines, in_lines, val_lines):
    width = dense_blocks.shape[2]

    def add_block(running, step_in):
        out_idx, in_idx, nz_vals, dense_blk = step_in
        picked = dense_blk[in_idx].astype(val_lines.dtype) * nz_vals[:, None]
        return running + jax.ops.segment_sum(picked, out_idx, num_segments=BLOCK_ROWS), None

    row_total, _ = lax.scan(add_block, jnp.zeros((BLOCK_ROWS, width), val_lines.dtype), (out_lines, in_lines, val_lines, dense_blocks))
    return row_total


def reference(a_rows, a_cols, a_vals, a_count, h_feat, w_mat, dz_out):
    live_mask = jnp.arange(NNZ_CAP, dtype=jnp.int32)[None, None, :] < a_count[:, :, None]
    live_vals = jnp.where(live_mask, a_vals, jnp.zeros((), a_vals.dtype))
    feat_blocks = h_feat.reshape(GRID_SIDE, BLOCK_ROWS, FEAT_IN)
    aggregate = lax.map(lambda block_in: block_sum(feat_blocks, block_in[0], block_in[1], block_in[2]), (a_rows, a_cols, live_vals)).reshape(NODES, FEAT_IN)
    aggregate_lo = aggregate.astype(jnp.bfloat16)
    pre_act = jnp.dot(aggregate_lo, w_mat, preferred_element_type=jnp.float32)
    z_out = jnp.maximum(pre_act, jnp.zeros((), pre_act.dtype))
    grad_pre = jnp.where(pre_act > 0, dz_out, jnp.zeros((), dz_out.dtype)).astype(jnp.bfloat16)
    dw_mat = jnp.dot(aggregate_lo.T, grad_pre, preferred_element_type=jnp.float32)
    grad_agg = jnp.dot(grad_pre, w_mat.T, preferred_element_type=jnp.float32).astype(jnp.bfloat16)
    grad_blocks = grad_agg.reshape(GRID_SIDE, BLOCK_ROWS, FEAT_IN)
    swapped = (jnp.swapaxes(a_cols, 0, 1), jnp.swapaxes(a_rows, 0, 1), jnp.swapaxes(live_vals, 0, 1))
    dh_feat = lax.map(lambda block_in: block_sum(grad_blocks, block_in[0], block_in[1], block_in[2]), swapped).reshape(NODES, FEAT_IN)
    return z_out, dw_mat, dh_feat
```

```python
import functools
import jax
import jax.numpy as jnp
from jax import lax
from jax.experimental import pallas as pl
from jax.experimental.pallas import tpu as pltpu
from jax.sharding import PartitionSpec as P

FEAT_PAD = 64
CHUNK = 4096
TILE = 1024
STEP = 128
BATCH = 4
N_ACC = 8


def line_address(node):
    return (node >> 3) * 16 + (node & 7)


def to_lines(dense):
    n = dense.shape[0]
    return dense.reshape(n // 8, 8, 2, 128).transpose(0, 2, 1, 3).reshape(2 * n, 128)


def from_lines(lines):
    n = lines.shape[0] // 2
    return lines.reshape(n // 8, 2, 8, 128).transpose(0, 2, 1, 3).reshape(n, 256)


def accumulate_kernel(ordered, cap, count_ref, clash_ref, in_hbm, out_hbm, vals_ref, table_ref, sum_ref, *scratch):
    n_acc = 1 if ordered else N_ACC
    accs = [sum_ref] + list(scratch[:n_acc - 1])
    in_s, out_s, spread, sems = scratch[n_acc - 1:]
    n_lines = sum_ref.shape[0]
    n_lists = count_ref.shape[0]
    lines_of = (lambda line: pl.ds(line, 1)) if ordered else (lambda line: pl.ds(line, 2, stride=8))
    width = 1 if ordered else 2

    def copies(start, slot):
        src, dst = pl.ds(start, CHUNK), pl.ds(slot * CHUNK, CHUNK)
        return (pltpu.make_async_copy(in_hbm.at[src], in_s.at[dst], sems.at[0, slot]),
                pltpu.make_async_copy(out_hbm.at[src], out_s.at[dst], sems.at[1, slot]))

    def clear(step, carry):
        lines = pl.ds(pl.multiple_of(step * 64, 64), 64)
        for acc in accs:
            acc[lines, :] = jnp.zeros((64, 128), jnp.float32)
        return carry

    lax.fori_loop(0, n_lines // 64, clear, 0)
    in_views = [in_s.at[pl.ds(off, 2 * CHUNK - STEP + 1)] for off in range(STEP)]
    out_views = [out_s.at[pl.ds(off, 2 * CHUNK - STEP + 1)] for off in range(STEP)]

    def take(step, base, batch_len):
        vals = spread.at[pl.ds(pl.multiple_of(step * STEP, STEP), STEP)]
        for first in range(0, STEP, batch_len):
            batch = []
            for u in range(batch_len):
                e = first + u
                src, dst = in_views[e][base], out_views[e][base]
                term = table_ref[lines_of(src), :] * jnp.broadcast_to(vals[e:e + 1, :], (width, 128))
                batch.append((dst, accs[u % n_acc][lines_of(dst), :] + term))
            for u in range(batch_len):
                accs[u % n_acc][lines_of(batch[u][0]), :] = batch[u][1]

    def list_body(which, carry):
        count = count_ref[which]
        n_chunks = (count + CHUNK - 1) // CHUNK
        for copy in copies(which * cap, 0):
            copy.start()

        def chunk_body(chunk, carry):
            slot = lax.rem(chunk, 2)
            start = which * cap + chunk * CHUNK
            for copy in copies(start, slot):
                copy.wait()

            @pl.when(chunk + 1 < n_chunks)
            def _():
                for copy in copies(start + CHUNK, 1 - slot):
                    copy.start()

            left = jnp.minimum(count - chunk * CHUNK, CHUNK)

            def tile_body(tile, carry):
                vals = vals_ref[pl.ds(pl.multiple_of(start // 128 + tile * 8, 8), 8), :]
                for j in range(128):
                    spread[8 * j:8 * j + 8, :] = jnp.broadcast_to(vals[:, j:j + 1], (8, 128))

                def step_body(step, carry):
                    base = slot * CHUNK + tile * TILE + step * STEP
                    if ordered:
                        clash = clash_ref[start // STEP + tile * (TILE // STEP) + step]

                        @pl.when(clash == 0)
                        def _():
                            take(step, base, BATCH)

                        @pl.when(clash != 0)
                        def _():
                            take(step, base, 1)
                    else:
                        take(step, base, n_acc)
                    return carry

                n_steps = (jnp.minimum(left - tile * TILE, TILE) + STEP - 1) // STEP
                lax.fori_loop(0, n_steps, step_body, 0)
                return carry

            lax.fori_loop(0, (left + TILE - 1) // TILE, tile_body, 0)
            return carry

        lax.fori_loop(0, n_chunks, chunk_body, 0)
        return carry

    lax.fori_loop(0, n_lists, list_body, 0)
    if not ordered:
        def finish(step, carry):
            lines = pl.ds(pl.multiple_of(step * 64, 64), 64)
            total = accs[0][lines, :]
            for acc in accs[1:]:
                total = total + acc[lines, :]
            sum_ref[lines, :] = total
            return carry

        lax.fori_loop(0, n_lines // 64, finish, 0)


def accumulate(ordered, count, clash, in_line, out_line, vals, table, n_lines):
    n_acc = 1 if ordered else N_ACC
    cap = in_line.shape[0] // count.shape[0]
    smem, vmem, anywhere = (pl.BlockSpec(memory_space=space) for space in (pltpu.SMEM, pltpu.VMEM, pl.ANY))
    return pl.pallas_call(
        functools.partial(accumulate_kernel, ordered, cap),
        out_shape=jax.ShapeDtypeStruct((n_lines, 128), jnp.float32),
        in_specs=[smem, smem, anywhere, anywhere, vmem, vmem],
        out_specs=vmem,
        scratch_shapes=[pltpu.VMEM((n_lines, 128), jnp.float32)] * (n_acc - 1)
        + [pltpu.SMEM((2 * CHUNK,), jnp.int32)] * 2
        + [pltpu.VMEM((TILE, 128), jnp.float32), pltpu.SemaphoreType.DMA((2, 2))],
        compiler_params=pltpu.CompilerParams(vmem_limit_bytes=(24 if ordered else 48) << 20),
        cost_estimate=pl.CostEstimate(flops=800_000_000, bytes_accessed=16 << 20, transcendentals=0),
        name="accumulate_ordered" if ordered else "accumulate",
    )(count, clash, in_line, out_line, vals, table)


def solution(mesh):
    side = mesh.shape['row']
    swap = [(a * side + b, b * side + a) for a in range(side) for b in range(side)]
    blk_spec = P(('graph', 'row'), 'col', None)
    row_spec = P(('graph', 'row'), 'col')

    def layer_local(rows_blk, cols_blk, vals_blk, count_blk, feat_blk, weight_blk, dz_blk):
        cap = rows_blk.shape[-1]
        n_rows, feat_part = feat_blk.shape
        rows, cols, count = rows_blk.reshape(cap), cols_blk.reshape(cap), count_blk.reshape(1)
        vals = jnp.where(jnp.arange(cap, dtype=jnp.int32) < count, vals_blk.reshape(cap), 0.0)
        vals = vals.reshape(cap // TILE, 128, 8).transpose(0, 2, 1).reshape(cap // 128, 128)
        lists = rows.reshape(cap // STEP, STEP)
        spot = jnp.arange(STEP, dtype=jnp.int32) % BATCH
        clash = jnp.zeros((cap // STEP,), jnp.int32)
        for gap in range(1, BATCH):
            same = (lists == jnp.roll(lists, gap, axis=1)) & (spot >= gap)
            clash = clash | jnp.any(same, axis=1).astype(jnp.int32)

        def gather_col(x):
            return lax.all_gather(x, 'col', axis=0, tiled=True)

        def pad_part(x, axis, size):
            pads = [(0, 0)] * x.ndim
            pads[axis] = (0, size - x.shape[axis])
            return jnp.pad(x, pads)

        notes = gather_col(jnp.concatenate([clash, jnp.broadcast_to(count, (128,))])).reshape(side, -1)
        weight = gather_col(pad_part(weight_blk, 0, FEAT_PAD))
        feat = lax.all_gather(pad_part(feat_blk, 1, FEAT_PAD), 'row', axis=0, tiled=True)
        table = pad_part(feat.astype(jnp.float32), 1, 128)
        rows_all, vals_all = gather_col(rows), gather_col(vals)
        cols_all = gather_col(cols + n_rows * lax.axis_index('col'))
        dz_lo = lax.all_to_all(dz_blk.astype(jnp.bfloat16), 'col', 0, 1, tiled=True)

        part_c = accumulate(True, notes[:, -1], notes[:, :-128].reshape(-1), cols_all, rows_all, vals_all, table, n_rows)
        aggregate_lo = lax.all_to_all(part_c[:, :FEAT_PAD].astype(jnp.bfloat16), 'col', 0, 1, tiled=True)
        pre_act = jnp.dot(aggregate_lo, weight, preferred_element_type=jnp.float32)
        grad_pre = jnp.where(pre_act > 0, dz_lo, jnp.zeros((), jnp.bfloat16))
        grad_agg = lax.dot_general(grad_pre, weight, (((1,), (1,)), ((), ())), preferred_element_type=jnp.float32).astype(jnp.bfloat16)
        grad_agg = lax.all_gather(grad_agg, 'col', axis=0, tiled=True)
        part_dh = accumulate(False, count, clash, line_address(rows), line_address(cols), vals, to_lines(grad_agg.astype(jnp.float32)), 2 * n_rows)

        z_blk = lax.all_to_all(jnp.maximum(pre_act, 0.0), 'col', 1, 0, tiled=True)
        part_dw = lax.dot_general(aggregate_lo, grad_pre, (((0,), (0,)), ((), ())), preferred_element_type=jnp.float32)
        part_dw = lax.psum_scatter(part_dw, 'col', scatter_dimension=0, tiled=True)
        dw_blk = lax.psum(part_dw, 'row')[:feat_part]

        dh = lax.psum_scatter(from_lines(part_dh), 'row', scatter_dimension=0, tiled=True)
        dh = lax.ppermute(dh, ('col', 'row'), swap)
        dh_blk = lax.all_to_all(dh, 'col', 1, 0, tiled=True)[:, :feat_part]
        return z_blk, dw_blk, dh_blk

    return jax.shard_map(layer_local, mesh=mesh, in_specs=(blk_spec, blk_spec, blk_spec, row_spec, row_spec, P('col', None), row_spec),
                         out_specs=(row_spec, P(('graph', 'col'), None), row_spec), check_vma=False)
```

```python
import functools
import jax
import jax.numpy as jnp
from jax import lax
from jax.experimental import pallas as pl
from jax.experimental.pallas import tpu as pltpu
from jax.sharding import PartitionSpec as P

FEAT_PAD = 64
CHUNK = 4096
TILE = 1024
STEP = 128
BATCHES = (8, 4, 2, 1)
N_ACC = 8


def line_address(node):
    return (node >> 3) * 16 + (node & 7)


def to_lines(dense):
    n = dense.shape[0]
    return dense.reshape(n // 8, 8, 2, 128).transpose(0, 2, 1, 3).reshape(2 * n, 128)


def from_lines(lines):
    n = lines.shape[0] // 2
    return lines.reshape(n // 8, 2, 8, 128).transpose(0, 2, 1, 3).reshape(n, 256)


def accumulate_kernel(ordered, cap, count_ref, level_ref, in_hbm, out_hbm, vals_ref, table_ref, sum_ref, *scratch):
    n_acc = 1 if ordered else N_ACC
    accs = [sum_ref] + list(scratch[:n_acc - 1])
    in_s, out_s, spread, sems = scratch[n_acc - 1:]
    n_lines = sum_ref.shape[0]
    n_lists = count_ref.shape[0]
    lines_of = (lambda line: pl.ds(line, 1)) if ordered else (lambda line: pl.ds(line, 2, stride=8))
    width = 1 if ordered else 2

    def copies(start, slot):
        src, dst = pl.ds(start, CHUNK), pl.ds(slot * CHUNK, CHUNK)
        return (pltpu.make_async_copy(in_hbm.at[src], in_s.at[dst], sems.at[0, slot]),
                pltpu.make_async_copy(out_hbm.at[src], out_s.at[dst], sems.at[1, slot]))

    def clear(step, carry):
        lines = pl.ds(pl.multiple_of(step * 64, 64), 64)
        for acc in accs:
            acc[lines, :] = jnp.zeros((64, 128), jnp.float32)
        return carry

    lax.fori_loop(0, n_lines // 64, clear, 0)
    in_views = [in_s.at[pl.ds(off, 2 * CHUNK - STEP + 1)] for off in range(STEP)]
    out_views = [out_s.at[pl.ds(off, 2 * CHUNK - STEP + 1)] for off in range(STEP)]

    def take(step, base, batch_len):
        vals = spread.at[pl.ds(pl.multiple_of(step * STEP, STEP), STEP)]
        for first in range(0, STEP, batch_len):
            batch = []
            for u in range(batch_len):
                e = first + u
                src, dst = in_views[e][base], out_views[e][base]
                term = table_ref[lines_of(src), :] * jnp.broadcast_to(vals[e:e + 1, :], (width, 128))
                batch.append((dst, accs[u % n_acc][lines_of(dst), :] + term))
            for u in range(batch_len):
                accs[u % n_acc][lines_of(batch[u][0]), :] = batch[u][1]

    def list_body(which, carry):
        count = count_ref[which]
        n_chunks = (count + CHUNK - 1) // CHUNK
        for copy in copies(which * cap, 0):
            copy.start()

        def chunk_body(chunk, carry):
            slot = lax.rem(chunk, 2)
            start = which * cap + chunk * CHUNK
            for copy in copies(start, slot):
                copy.wait()

            @pl.when(chunk + 1 < n_chunks)
            def _():
                for copy in copies(start + CHUNK, 1 - slot):
                    copy.start()

            left = jnp.minimum(count - chunk * CHUNK, CHUNK)

            def tile_body(tile, carry):
                vals = vals_ref[pl.ds(pl.multiple_of(start // 128 + tile * 8, 8), 8), :]
                for j in range(128):
                    spread[8 * j:8 * j + 8, :] = jnp.broadcast_to(vals[:, j:j + 1], (8, 128))

                def step_body(step, carry):
                    base = slot * CHUNK + tile * TILE + step * STEP
                    if ordered:
                        level = level_ref[start // STEP + tile * (TILE // STEP) + step]
                        for at, batch_len in enumerate(BATCHES):
                            @pl.when(level == at)
                            def _(batch_len=batch_len):
                                take(step, base, batch_len)
                    else:
                        take(step, base, n_acc)
                    return carry

                n_steps = (jnp.minimum(left - tile * TILE, TILE) + STEP - 1) // STEP
                lax.fori_loop(0, n_steps, step_body, 0)
                return carry

            lax.fori_loop(0, (left + TILE - 1) // TILE, tile_body, 0)
            return carry

        lax.fori_loop(0, n_chunks, chunk_body, 0)
        return carry

    lax.fori_loop(0, n_lists, list_body, 0)
    if not ordered:
        def finish(step, carry):
            lines = pl.ds(pl.multiple_of(step * 64, 64), 64)
            total = accs[0][lines, :]
            for acc in accs[1:]:
                total = total + acc[lines, :]
            sum_ref[lines, :] = total
            return carry

        lax.fori_loop(0, n_lines // 64, finish, 0)


def accumulate(ordered, count, level, in_line, out_line, vals, table, n_lines):
    n_acc = 1 if ordered else N_ACC
    cap = in_line.shape[0] // count.shape[0]
    smem, vmem, anywhere = (pl.BlockSpec(memory_space=space) for space in (pltpu.SMEM, pltpu.VMEM, pl.ANY))
    return pl.pallas_call(
        functools.partial(accumulate_kernel, ordered, cap),
        out_shape=jax.ShapeDtypeStruct((n_lines, 128), jnp.float32),
        in_specs=[smem, smem, anywhere, anywhere, vmem, vmem],
        out_specs=vmem,
        scratch_shapes=[pltpu.VMEM((n_lines, 128), jnp.float32)] * (n_acc - 1)
        + [pltpu.SMEM((2 * CHUNK,), jnp.int32)] * 2
        + [pltpu.VMEM((TILE, 128), jnp.float32), pltpu.SemaphoreType.DMA((2, 2))],
        compiler_params=pltpu.CompilerParams(vmem_limit_bytes=(24 if ordered else 48) << 20),
        cost_estimate=pl.CostEstimate(flops=800_000_000, bytes_accessed=16 << 20, transcendentals=0),
        name="accumulate_ordered" if ordered else "accumulate",
    )(count, level, in_line, out_line, vals, table)


def batch_levels(nodes):
    lists = nodes.reshape(-1, 128)
    spot = jnp.arange(128, dtype=jnp.int32)
    clash = jnp.zeros(lists.shape, jnp.int32)
    for at, batch_len in enumerate(BATCHES[:-1]):
        for gap in range(1, batch_len):
            same = (lists == jnp.roll(lists, gap, axis=1)) & (spot % batch_len >= gap)
            clash = jnp.where(same, at + 1, clash)
    per_step = [jnp.max(jnp.where(spot // STEP == part, clash, 0), axis=1) for part in range(128 // STEP)]
    return jnp.stack(per_step, axis=1).reshape(-1)


def solution(mesh):
    side = mesh.shape['row']
    swap = [(a * side + b, b * side + a) for a in range(side) for b in range(side)]
    blk_spec = P(('graph', 'row'), 'col', None)
    row_spec = P(('graph', 'row'), 'col')

    def layer_local(rows_blk, cols_blk, vals_blk, count_blk, feat_blk, weight_blk, dz_blk):
        cap = rows_blk.shape[-1]
        n_rows, feat_part = feat_blk.shape
        rows, cols, count = rows_blk.reshape(cap), cols_blk.reshape(cap), count_blk.reshape(1)
        vals = jnp.where(jnp.arange(cap, dtype=jnp.int32) < count, vals_blk.reshape(cap), 0.0)
        vals = vals.reshape(cap // TILE, 128, 8).transpose(0, 2, 1).reshape(cap // 128, 128)
        def gather_col(x):
            return lax.all_gather(x, 'col', axis=0, tiled=True)

        def pad_part(x, axis, size):
            pads = [(0, 0)] * x.ndim
            pads[axis] = (0, size - x.shape[axis])
            return jnp.pad(x, pads)

        feat = lax.all_gather(pad_part(feat_blk, 1, FEAT_PAD), 'row', axis=0, tiled=True)
        table = pad_part(feat.astype(jnp.float32), 1, 128)
        places = gather_col(rows | ((cols + n_rows * lax.axis_index('col')) << 16))
        vals_all = gather_col(vals)
        counts = gather_col(jnp.broadcast_to(count, (1, 128)))[:, 0]
        weight = gather_col(pad_part(weight_blk, 0, FEAT_PAD))
        rows_all, cols_all = places & 0xFFFF, places >> 16
        level = batch_levels(rows_all)
        dz_lo = lax.all_to_all(dz_blk.astype(jnp.bfloat16), 'col', 0, 1, tiled=True)

        table, weight, dz_lo = lax.optimization_barrier((table, weight, dz_lo))
        part_c = accumulate(True, counts, level, cols_all, rows_all, vals_all, table, n_rows)
        aggregate_lo = lax.all_to_all(part_c[:, :FEAT_PAD].astype(jnp.bfloat16), 'col', 0, 1, tiled=True)
        pre_act = jnp.dot(aggregate_lo, weight, preferred_element_type=jnp.float32)
        grad_pre = jnp.where(pre_act > 0, dz_lo, jnp.zeros((), jnp.bfloat16))
        grad_agg = lax.dot_general(grad_pre, weight, (((1,), (1,)), ((), ())), preferred_element_type=jnp.float32).astype(jnp.bfloat16)
        part_dw = lax.dot_general(aggregate_lo, grad_pre, (((0,), (0,)), ((), ())), preferred_element_type=jnp.float32)
        grad_agg = lax.all_gather(grad_agg, 'col', axis=0, tiled=True)
        grad_agg, part_dw, z_rows = lax.optimization_barrier((grad_agg, part_dw, jnp.maximum(pre_act, 0.0)))
        z_blk = lax.all_to_all(z_rows, 'col', 1, 0, tiled=True)
        dw_all = lax.psum(part_dw, ('col', 'row'))
        part_dh = accumulate(False, count, jnp.zeros((1,), jnp.int32), line_address(rows), line_address(cols), vals,
                             to_lines(grad_agg.astype(jnp.float32)), 2 * n_rows)
        part_dh, z_blk, dw_all = lax.optimization_barrier((part_dh, z_blk, dw_all))
        dw_blk = lax.dynamic_slice_in_dim(dw_all, lax.axis_index('col') * FEAT_PAD, feat_part, axis=0)
        dh = lax.psum_scatter(from_lines(part_dh), 'row', scatter_dimension=0, tiled=True)
        dh = lax.ppermute(dh, ('col', 'row'), swap)
        dh_blk = lax.all_to_all(dh, 'col', 1, 0, tiled=True)[:, :feat_part]
        return z_blk, dw_blk, dh_blk

    return jax.shard_map(layer_local, mesh=mesh, in_specs=(blk_spec, blk_spec, blk_spec, row_spec, row_spec, P('col', None), row_spec),
                         out_specs=(row_spec, P(('graph', 'col'), None), row_spec), check_vma=False)
```

```python
import functools
import jax
import jax.numpy as jnp
from jax import lax
from jax.experimental import pallas as pl
from jax.experimental.pallas import tpu as pltpu
from jax.sharding import PartitionSpec as P

FEAT_PAD = 64
CHUNK = 4096
STEP = 128
BATCHES = (8, 4, 2, 1)
N_ACC = 8


def line_address(node):
    return (node >> 3) * 16 + (node & 7)


def to_lines(dense):
    n = dense.shape[0]
    return dense.reshape(n // 8, 8, 2, 128).transpose(0, 2, 1, 3).reshape(2 * n, 128)


def from_lines(lines):
    n = lines.shape[0] // 2
    return lines.reshape(n // 8, 2, 8, 128).transpose(0, 2, 1, 3).reshape(n, 256)


def accumulate_kernel(ordered, cap, vals_at, count_ref, level_ref, in_hbm, out_hbm, vals_hbm, table_ref, sum_ref, *scratch):
    n_acc = 1 if ordered else N_ACC
    accs = [sum_ref] + list(scratch[:n_acc - 1])
    in_s, out_s, vals_s, sems = scratch[n_acc - 1:]
    n_lines = sum_ref.shape[0]
    n_lists = count_ref.shape[0]
    lines_of = (lambda line: pl.ds(line, 1)) if ordered else (lambda line: pl.ds(line, 2, stride=8))

    def copies(which, chunk, slot):
        src, dst = pl.ds(which * cap + chunk * CHUNK, CHUNK), pl.ds(slot * CHUNK, CHUNK)
        first, stride = vals_at
        vals_src = pl.ds(first + which * stride + chunk * CHUNK, CHUNK)
        return (pltpu.make_async_copy(in_hbm.at[src], in_s.at[dst], sems.at[0, slot]),
                pltpu.make_async_copy(out_hbm.at[src], out_s.at[dst], sems.at[1, slot]),
                pltpu.make_async_copy(vals_hbm.at[vals_src], vals_s.at[dst], sems.at[2, slot]))

    def clear(step, carry):
        lines = pl.ds(pl.multiple_of(step * 64, 64), 64)
        for acc in accs:
            acc[lines, :] = jnp.zeros((64, 128), jnp.float32)
        return carry

    lax.fori_loop(0, n_lines // 64, clear, 0)
    in_views, out_views, vals_views = (
        [ref.at[pl.ds(off, 2 * CHUNK - STEP + 1)] for off in range(STEP)] for ref in (in_s, out_s, vals_s))

    def take(base, batch_len):
        for first in range(0, STEP, batch_len):
            batch = []
            for u in range(batch_len):
                e = first + u
                src, dst, val = in_views[e][base], out_views[e][base], vals_views[e][base]
                batch.append((dst, accs[u % n_acc][lines_of(dst), :] + table_ref[lines_of(src), :] * val))
            for u in range(batch_len):
                accs[u % n_acc][lines_of(batch[u][0]), :] = batch[u][1]

    def list_body(which, carry):
        count = count_ref[which]
        n_chunks = (count + CHUNK - 1) // CHUNK
        for copy in copies(which, 0, 0):
            copy.start()

        def chunk_body(chunk, carry):
            slot = lax.rem(chunk, 2)
            for copy in copies(which, chunk, slot):
                copy.wait()

            @pl.when(chunk + 1 < n_chunks)
            def _():
                for copy in copies(which, chunk + 1, 1 - slot):
                    copy.start()

            left = jnp.minimum(count - chunk * CHUNK, CHUNK)

            def step_body(step, carry):
                base = slot * CHUNK + step * STEP
                if ordered:
                    level = level_ref[which * (cap // STEP) + chunk * (CHUNK // STEP) + step]
                    for at, batch_len in enumerate(BATCHES):
                        @pl.when(level == at)
                        def _(batch_len=batch_len):
                            take(base, batch_len)
                else:
                    take(base, n_acc)
                return carry

            lax.fori_loop(0, (left + STEP - 1) // STEP, step_body, 0)
            return carry

        lax.fori_loop(0, n_chunks, chunk_body, 0)
        return carry

    lax.fori_loop(0, n_lists, list_body, 0)
    if not ordered:
        def finish(step, carry):
            lines = pl.ds(pl.multiple_of(step * 64, 64), 64)
            total = accs[0][lines, :]
            for acc in accs[1:]:
                total = total + acc[lines, :]
            sum_ref[lines, :] = total
            return carry

        lax.fori_loop(0, n_lines // 64, finish, 0)


def accumulate(ordered, count, level, in_line, out_line, vals, table, n_lines, vals_at=(0, 0)):
    n_acc = 1 if ordered else N_ACC
    cap = in_line.shape[0] // count.shape[0]
    smem, vmem, anywhere = (pl.BlockSpec(memory_space=space) for space in (pltpu.SMEM, pltpu.VMEM, pl.ANY))
    return pl.pallas_call(
        functools.partial(accumulate_kernel, ordered, cap, vals_at),
        out_shape=jax.ShapeDtypeStruct((n_lines, 128), jnp.float32),
        in_specs=[smem, smem, anywhere, anywhere, anywhere, vmem],
        out_specs=vmem,
        scratch_shapes=[pltpu.VMEM((n_lines, 128), jnp.float32)] * (n_acc - 1)
        + [pltpu.SMEM((2 * CHUNK,), jnp.int32)] * 2
        + [pltpu.SMEM((2 * CHUNK,), jnp.float32), pltpu.SemaphoreType.DMA((3, 2))],
        compiler_params=pltpu.CompilerParams(vmem_limit_bytes=(24 if ordered else 48) << 20),
        cost_estimate=pl.CostEstimate(flops=800_000_000, bytes_accessed=16 << 20, transcendentals=0),
        name="accumulate_ordered" if ordered else "accumulate",
    )(count, level, in_line, out_line, vals, table)


def batch_levels(nodes):
    lists = nodes.reshape(-1, 128)
    spot = jnp.arange(128, dtype=jnp.int32)
    clash = jnp.zeros(lists.shape, jnp.int32)
    for at, batch_len in enumerate(BATCHES[:-1]):
        for gap in range(1, batch_len):
            same = (lists == jnp.roll(lists, gap, axis=1)) & (spot % batch_len >= gap)
            clash = jnp.where(same, at + 1, clash)
    per_step = [jnp.max(jnp.where(spot // STEP == part, clash, 0), axis=1) for part in range(128 // STEP)]
    return jnp.stack(per_step, axis=1).reshape(-1)


def solution(mesh):
    side = mesh.shape['row']
    blk_spec = P(('graph', 'row'), 'col', None)
    row_spec = P(('graph', 'row'), 'col')

    def layer_local(rows_blk, cols_blk, vals_blk, count_blk, feat_blk, weight_blk, dz_blk):
        cap = rows_blk.shape[-1]
        n_rows, feat_part = feat_blk.shape
        rows, cols, count = rows_blk.reshape(cap), cols_blk.reshape(cap), count_blk.reshape(1)
        vals = jnp.where(jnp.arange(cap, dtype=jnp.int32) < count, vals_blk.reshape(cap), 0.0)
        def gather_col(x):
            return lax.all_gather(x, 'col', axis=0, tiled=True)

        def pad_part(x, axis, size):
            pads = [(0, 0)] * x.ndim
            pads[axis] = (0, size - x.shape[axis])
            return jnp.pad(x, pads)

        feat = lax.all_gather(pad_part(feat_blk, 1, FEAT_PAD), 'row', axis=0, tiled=True)
        table = pad_part(feat.astype(jnp.float32), 1, 128)
        place = (rows + n_rows * cols).astype(jnp.float32)
        one_list = jnp.concatenate([place, vals, jnp.broadcast_to(count.astype(jnp.float32), (1024,))])
        lists = gather_col(one_list)
        stride = one_list.shape[0]
        places = [lists[k * stride:k * stride + cap].astype(jnp.int32) for k in range(side)]
        counts = jnp.stack([lists[k * stride + 2 * cap] for k in range(side)]).astype(jnp.int32)
        weight = gather_col(pad_part(weight_blk, 0, FEAT_PAD))
        rows_all = jnp.concatenate([lax.rem(place, n_rows) for place in places])
        cols_all = jnp.concatenate([lax.div(place, n_rows) + k * n_rows for k, place in enumerate(places)])
        level = batch_levels(rows_all)
        dz_lo = lax.all_to_all(dz_blk.astype(jnp.bfloat16), 'col', 0, 1, tiled=True)

        table, weight, dz_lo = lax.optimization_barrier((table, weight, dz_lo))
        part_c = accumulate(True, counts, level, cols_all, rows_all, lists, table, n_rows, (cap, stride))
        aggregate_lo = lax.all_to_all(part_c[:, :FEAT_PAD].astype(jnp.bfloat16), 'col', 0, 1, tiled=True)
        pre_act = jnp.dot(aggregate_lo, weight, preferred_element_type=jnp.float32)
        grad_pre = jnp.where(pre_act > 0, dz_lo, jnp.zeros((), jnp.bfloat16))
        grad_agg = lax.dot_general(grad_pre, weight, (((1,), (1,)), ((), ())), preferred_element_type=jnp.float32).astype(jnp.bfloat16)
        part_dw = lax.dot_general(aggregate_lo, grad_pre, (((0,), (0,)), ((), ())), preferred_element_type=jnp.float32)
        turns = [[((pos + turn) % side, pos) for pos in range(side)] for turn in range(1, side)]
        grad_agg = jnp.concatenate([grad_agg] + [lax.ppermute(grad_agg, 'col', turn) for turn in turns], axis=0)
        quarter = n_rows // side
        turned = (rows // quarter + side - lax.axis_index('col')) % side * quarter + rows % quarter
        grad_agg, part_dw, z_rows = lax.optimization_barrier((grad_agg, part_dw, jnp.maximum(pre_act, 0.0)))
        z_blk = lax.all_to_all(z_rows, 'col', 1, 0, tiled=True)
        dw_all = lax.psum(part_dw, ('col', 'row'))
        part_dh = accumulate(False, count, jnp.zeros((1,), jnp.int32), line_address(turned), line_address(cols), vals,
                             to_lines(grad_agg.astype(jnp.float32)), 2 * n_rows)
        part_dh, z_blk, dw_all = lax.optimization_barrier((part_dh, z_blk, dw_all))
        dw_blk = lax.dynamic_slice_in_dim(dw_all, lax.axis_index('col') * FEAT_PAD, feat_part, axis=0)
        dh = lax.psum_scatter(from_lines(part_dh), 'row', scatter_dimension=0, tiled=True)
        pieces = dh.reshape(quarter, side, FEAT_PAD).transpose(1, 0, 2)
        dh_blk = jnp.zeros((n_rows, FEAT_PAD), jnp.float32)
        for turn in range(side):
            piece = lax.dynamic_index_in_dim(pieces, (lax.axis_index('row') + turn) % side, keepdims=False)
            moves = [(k * side + p, (p + turn) % side * side + k) for p in range(side) for k in range(side)]
            piece = lax.ppermute(piece, ('col', 'row'), moves)
            origin = (lax.axis_index('col') + side - turn) % side
            dh_blk = lax.dynamic_update_slice_in_dim(dh_blk, piece, origin * quarter, axis=0)
        dh_blk = dh_blk[:, :feat_part]
        return z_blk, dw_blk, dh_blk

    return jax.shard_map(layer_local, mesh=mesh, in_specs=(blk_spec, blk_spec, blk_spec, row_spec, row_spec, P('col', None), row_spec),
                         out_specs=(row_spec, P(('graph', 'col'), None), row_spec), check_vma=False)
```

```python
import functools
import jax
import jax.numpy as jnp
from jax import lax
from jax.experimental import pallas as pl
from jax.experimental.pallas import tpu as pltpu
from jax.sharding import PartitionSpec as P

FEAT_PAD = 64
CHUNK = 4096
STEP = 128
BATCHES = (8, 4, 2, 1)
N_ACC = 8


def line_address(node):
    return (node >> 3) * 16 + (node & 7)


def to_lines(dense):
    n = dense.shape[0]
    return dense.reshape(n // 8, 8, 2, 128).transpose(0, 2, 1, 3).reshape(2 * n, 128)


def from_lines(lines):
    n = lines.shape[0] // 2
    return lines.reshape(n // 8, 2, 8, 128).transpose(0, 2, 1, 3).reshape(n, 256)


def accumulate_kernel(ordered, cap, vals_at, count_ref, level_ref, in_hbm, out_hbm, vals_hbm, table_ref, sum_ref, *scratch):
    n_acc = 1 if ordered else N_ACC
    accs = [sum_ref] + list(scratch[:n_acc - 1])
    in_s, out_s, vals_s, sems = scratch[n_acc - 1:]
    n_lines = sum_ref.shape[0]
    n_lists = count_ref.shape[0]
    lines_of = (lambda line: pl.ds(line, 1)) if ordered else (lambda line: pl.ds(line, 2, stride=8))

    def copies(which, chunk, slot):
        src, dst = pl.ds(which * cap + chunk * CHUNK, CHUNK), pl.ds(slot * CHUNK, CHUNK)
        first, stride = vals_at
        vals_src = pl.ds(first + which * stride + chunk * CHUNK, CHUNK)
        return (pltpu.make_async_copy(in_hbm.at[src], in_s.at[dst], sems.at[0, slot]),
                pltpu.make_async_copy(out_hbm.at[src], out_s.at[dst], sems.at[1, slot]),
                pltpu.make_async_copy(vals_hbm.at[vals_src], vals_s.at[dst], sems.at[2, slot]))

    def clear(step, carry):
        lines = pl.ds(pl.multiple_of(step * 64, 64), 64)
        for acc in accs:
            acc[lines, :] = jnp.zeros((64, 128), jnp.float32)
        return carry

    lax.fori_loop(0, n_lines // 64, clear, 0)
    in_views, out_views, vals_views = (
        [ref.at[pl.ds(off, 2 * CHUNK - STEP + 1)] for off in range(STEP)] for ref in (in_s, out_s, vals_s))

    def take(base, batch_len):
        for first in range(0, STEP, batch_len):
            batch = []
            for u in range(batch_len):
                e = first + u
                src, dst, val = in_views[e][base], out_views[e][base], vals_views[e][base]
                batch.append((dst, accs[u % n_acc][lines_of(dst), :] + table_ref[lines_of(src), :] * val))
            for u in range(batch_len):
                accs[u % n_acc][lines_of(batch[u][0]), :] = batch[u][1]

    def list_body(which, carry):
        count = count_ref[which]
        n_chunks = (count + CHUNK - 1) // CHUNK
        for copy in copies(which, 0, 0):
            copy.start()

        def chunk_body(chunk, carry):
            slot = lax.rem(chunk, 2)
            for copy in copies(which, chunk, slot):
                copy.wait()

            @pl.when(chunk + 1 < n_chunks)
            def _():
                for copy in copies(which, chunk + 1, 1 - slot):
                    copy.start()

            left = jnp.minimum(count - chunk * CHUNK, CHUNK)

            def step_body(step, carry):
                base = slot * CHUNK + step * STEP
                if ordered:
                    level = level_ref[which * (cap // STEP) + chunk * (CHUNK // STEP) + step]
                    for at, batch_len in enumerate(BATCHES):
                        @pl.when(level == at)
                        def _(batch_len=batch_len):
                            take(base, batch_len)
                else:
                    take(base, n_acc)
                return carry

            lax.fori_loop(0, (left + STEP - 1) // STEP, step_body, 0)
            return carry

        lax.fori_loop(0, n_chunks, chunk_body, 0)
        return carry

    lax.fori_loop(0, n_lists, list_body, 0)
    if not ordered:
        def finish(step, carry):
            lines = pl.ds(pl.multiple_of(step * 64, 64), 64)
            total = accs[0][lines, :]
            for acc in accs[1:]:
                total = total + acc[lines, :]
            sum_ref[lines, :] = total
            return carry

        lax.fori_loop(0, n_lines // 64, finish, 0)


def accumulate(ordered, count, level, in_line, out_line, vals, table, n_lines, vals_at=(0, 0)):
    n_acc = 1 if ordered else N_ACC
    cap = in_line.shape[0] // count.shape[0]
    smem, vmem, anywhere = (pl.BlockSpec(memory_space=space) for space in (pltpu.SMEM, pltpu.VMEM, pl.ANY))
    return pl.pallas_call(
        functools.partial(accumulate_kernel, ordered, cap, vals_at),
        out_shape=jax.ShapeDtypeStruct((n_lines, 128), jnp.float32),
        in_specs=[smem, smem, anywhere, anywhere, anywhere, vmem],
        out_specs=vmem,
        scratch_shapes=[pltpu.VMEM((n_lines, 128), jnp.float32)] * (n_acc - 1)
        + [pltpu.SMEM((2 * CHUNK,), jnp.int32)] * 2
        + [pltpu.SMEM((2 * CHUNK,), jnp.float32), pltpu.SemaphoreType.DMA((3, 2))],
        compiler_params=pltpu.CompilerParams(vmem_limit_bytes=(24 if ordered else 48) << 20),
        cost_estimate=pl.CostEstimate(flops=800_000_000, bytes_accessed=16 << 20, transcendentals=0),
        name="accumulate_ordered" if ordered else "accumulate",
    )(count, level, in_line, out_line, vals, table)


def batch_levels(nodes):
    lists = nodes.reshape(-1, 128)
    spot = jnp.arange(128, dtype=jnp.int32)
    clash = jnp.zeros(lists.shape, jnp.int32)
    for at, batch_len in enumerate(BATCHES[:-1]):
        for gap in range(1, batch_len):
            same = (lists == jnp.roll(lists, gap, axis=1)) & (spot % batch_len >= gap)
            clash = jnp.where(same, at + 1, clash)
    per_step = [jnp.max(jnp.where(spot // STEP == part, clash, 0), axis=1) for part in range(128 // STEP)]
    return jnp.stack(per_step, axis=1).reshape(-1)


def solution(mesh):
    side = mesh.shape['row']
    blk_spec = P(('graph', 'row'), 'col', None)
    row_spec = P(('graph', 'row'), 'col')

    def layer_local(rows_blk, cols_blk, vals_blk, count_blk, feat_blk, weight_blk, dz_blk):
        cap = rows_blk.shape[-1]
        n_rows, feat_part = feat_blk.shape
        rows, cols, count = rows_blk.reshape(cap), cols_blk.reshape(cap), count_blk.reshape(1)
        vals = jnp.where(jnp.arange(cap, dtype=jnp.int32) < count, vals_blk.reshape(cap), 0.0)
        def gather_col(x):
            return lax.all_gather(x, 'col', axis=0, tiled=True)

        def pad_part(x, axis, size):
            pads = [(0, 0)] * x.ndim
            pads[axis] = (0, size - x.shape[axis])
            return jnp.pad(x, pads)

        turns = [[((pos + turn) % side, pos) for pos in range(side)] for turn in range(1, side)]
        half = n_rows // 2
        feat = pad_part(feat_blk, 1, FEAT_PAD)
        feat = jnp.concatenate([feat[:half], feat[half:]], axis=1)
        feat = [feat] + [lax.ppermute(feat, 'row', turn) for turn in turns]
        feat = jnp.concatenate([part[:, side_of:side_of + FEAT_PAD] for part in feat for side_of in (0, FEAT_PAD)], axis=0)
        table = pad_part(feat.astype(jnp.float32), 1, 128)
        place = (rows + n_rows * cols).astype(jnp.float32)
        one_list = jnp.concatenate([place, vals, jnp.broadcast_to(count.astype(jnp.float32), (1024,))])
        lists = gather_col(one_list)
        stride = one_list.shape[0]
        places = [lists[k * stride:k * stride + cap].astype(jnp.int32) for k in range(side)]
        counts = jnp.stack([lists[k * stride + 2 * cap] for k in range(side)]).astype(jnp.int32)
        weight = gather_col(pad_part(weight_blk, 0, FEAT_PAD))
        rows_all = jnp.concatenate([lax.rem(place, n_rows) for place in places])
        cols_all = jnp.concatenate([lax.div(place, n_rows) + (k + side - lax.axis_index('row')) % side * n_rows
                                    for k, place in enumerate(places)])
        level = batch_levels(rows_all)
        dz_lo = lax.all_to_all(dz_blk.astype(jnp.bfloat16), 'col', 0, 1, tiled=True)

        table, weight, dz_lo = lax.optimization_barrier((table, weight, dz_lo))
        part_c = accumulate(True, counts, level, cols_all, rows_all, lists, table, n_rows, (cap, stride))
        aggregate_lo = lax.all_to_all(part_c[:, :FEAT_PAD].astype(jnp.bfloat16), 'col', 0, 1, tiled=True)
        pre_act = jnp.dot(aggregate_lo, weight, preferred_element_type=jnp.float32)
        grad_pre = jnp.where(pre_act > 0, dz_lo, jnp.zeros((), jnp.bfloat16))
        grad_agg = lax.dot_general(grad_pre, weight, (((1,), (1,)), ((), ())), preferred_element_type=jnp.float32).astype(jnp.bfloat16)
        part_dw = lax.dot_general(aggregate_lo, grad_pre, (((0,), (0,)), ((), ())), preferred_element_type=jnp.float32)
        grad_agg = jnp.concatenate([grad_agg] + [lax.ppermute(grad_agg, 'col', turn) for turn in turns], axis=0)
        quarter = n_rows // side
        turned = (rows // quarter + side - lax.axis_index('col')) % side * quarter + rows % quarter
        grad_agg, part_dw, z_rows = lax.optimization_barrier((grad_agg, part_dw, jnp.maximum(pre_act, 0.0)))
        z_blk = lax.all_to_all(z_rows, 'col', 1, 0, tiled=True)
        dw_all = lax.psum(part_dw, ('col', 'row'))
        part_dh = accumulate(False, count, jnp.zeros((1,), jnp.int32), line_address(turned), line_address(cols), vals,
                             to_lines(grad_agg.astype(jnp.float32)), 2 * n_rows)
        part_dh, z_blk, dw_all = lax.optimization_barrier((part_dh, z_blk, dw_all))
        dw_blk = lax.dynamic_slice_in_dim(dw_all, lax.axis_index('col') * FEAT_PAD, feat_part, axis=0)
        dh = lax.psum_scatter(from_lines(part_dh), 'row', scatter_dimension=0, tiled=True)
        pieces = dh.reshape(quarter, side, FEAT_PAD).transpose(1, 0, 2)
        dh_blk = jnp.zeros((n_rows, FEAT_PAD), jnp.float32)
        for turn in range(side):
            piece = lax.dynamic_index_in_dim(pieces, (lax.axis_index('row') + turn) % side, keepdims=False)
            moves = [(k * side + p, (p + turn) % side * side + k) for p in range(side) for k in range(side)]
            piece = lax.ppermute(piece, ('col', 'row'), moves)
            origin = (lax.axis_index('col') + side - turn) % side
            dh_blk = lax.dynamic_update_slice_in_dim(dh_blk, piece, origin * quarter, axis=0)
        dh_blk = dh_blk[:, :feat_part]
        return z_blk, dw_blk, dh_blk

    return jax.shard_map(layer_local, mesh=mesh, in_specs=(blk_spec, blk_spec, blk_spec, row_spec, row_spec, P('col', None), row_spec),
                         out_specs=(row_spec, P(('graph', 'col'), None), row_spec), check_vma=False)
```
